32 devices in a mesh: dom: 16 (over z, y, x), mp: 2 (over core).
Axes of the slice: x: 2, y: 2, z: 4, core: 2. Of those that a mesh axis runs over, the one named last changes fastest.
Arguments:
- table: bfloat16 [65536, 768], P('dom', 'mp'), may hold values from -6 to 6
- weight_a: bfloat16 [1536, 512], P(None, 'mp'), may hold values from -0.15625 to 0.15625
- bias_a: float32 [512], replicated, may hold values from -3 to 3
- weight_b: bfloat16 [1024, 512], P(None, 'mp'), may hold values from -0.25 to 0.25
- bias_b: float32 [512], replicated, may hold values from -3 to 3
- requests: int32 [16, 16, 128], P('dom'), may hold values from 0 to 4095
- near_a: int32 [16384, 10], P('dom'), may hold values from 0 to 2047
- self_a: int32 [16384], P('dom'), may hold values from 0 to 2047
- count_a: int32 [16384], P('dom'), may hold values from 1 to 10
- near_b: int32 [4096, 5], P('dom'), may hold values from 0 to 1023
- self_b: int32 [4096], P('dom'), may hold values from 0 to 1023
- count_b: int32 [4096], P('dom'), may hold values from 1 to 5
Outputs:
- embedding: bfloat16 [4096, 512], P('dom', 'mp')
The draws below stay inside these ranges and needn't reach their ends.
Inputs may be any that keep to these rules, and one draw needn't show every extreme that they name: `requests`: local row indices at the owner. `near_a`: slots of the same minibatch; entries at j >= count_a are padding. `near_b`: positions within the same minibatch; entries at j >= count_b are padding.
All inputs are finite; a program needn't handle non-finite values.
Results may differ from the reference program's by a relative error of at most 0.0074.
Values may be sent and summed in bfloat16 or wider, within the bound.
A program may use at most 64 MiB of HBM per device.

```python
import jax
import jax.numpy as jnp
from jax import lax

F = 768
H = 512
FAN_A = 10
FAN_B = 5
SEEDS_DEV = 256
NODE_DEV = 4096
HOP_DEV = 1024
SLOTS_DEV = 2048
NODES = 65536
HOPS = 16384
SEEDS = 4096
N_DOM = 16


def set_ends(values, stream_key, smallest, high):
    index_at = [jax.random.randint(jax.random.fold_in(stream_key, axis), (), 0, length) for axis, length in enumerate(values.shape)]
    widest = values.shape.index(max(values.shape))
    beside = index_at[:widest] + [(index_at[widest] + 1) % values.shape[widest]] + index_at[widest + 1:]
    return values.at[tuple(index_at)].set(smallest).at[tuple(beside)].set(high)


def level_of(rng, dims, split, smallest, high):
    def one(axis_at, blocks):
        heights = jax.random.uniform(jax.random.fold_in(jax.random.fold_in(rng, 6), axis_at), (blocks,), jnp.float32, smallest / len(split), high / len(split))
        return jnp.repeat(jnp.exp(heights), dims[axis_at] // blocks).reshape((-1,) + (1,) * (len(dims) - axis_at - 1))

    level = one(*split[0])
    for cut in split[1:]:
        level = level * one(*cut)
    return level


def centred(rng, dims, width, most, shards=(), kind=jnp.bfloat16):
    loudness = level_of(rng, dims, shards, -0.22, 0.18) if shards else 1.0
    values = jax.random.normal(rng, dims, jnp.float32) * width * loudness
    return jnp.minimum(jnp.maximum(values, -most), most).astype(kind)


def setup_inputs(seed: int = 0) -> dict:
    splits = jax.random.split(jax.random.key(seed), 13)
    table = centred(splits[0], (NODES, F), 1.0, 6.0, ((0, 16), (1, 2)))
    weight_a = centred(splits[1], (2 * F, H), (2 * F) ** -0.5, 0.15625, ((1, 2),))
    bias_a = centred(splits[2], (H,), 0.5, 3.0, (), jnp.float32)
    weight_b = centred(splits[3], (2 * H, H), H ** -0.5, 0.25, ((1, 2),))
    bias_b = centred(splits[4], (H,), 0.5, 3.0, (), jnp.float32)
    requests = set_ends(jax.random.randint(splits[5], (N_DOM, N_DOM, SLOTS_DEV // N_DOM), 0, NODE_DEV), jax.random.fold_in(splits[5], 1), 0, NODE_DEV - 1).astype(jnp.int32)
    near_a = set_ends(jax.random.randint(splits[6], (HOPS, FAN_A), 0, SLOTS_DEV), jax.random.fold_in(splits[6], 1), 0, SLOTS_DEV - 1).astype(jnp.int32)
    self_a = set_ends(jax.random.randint(splits[7], (HOPS,), 0, SLOTS_DEV), jax.random.fold_in(splits[7], 1), 0, SLOTS_DEV - 1).astype(jnp.int32)
    count_a = set_ends(jax.random.randint(splits[8], (HOPS,), 1, FAN_A + 1), jax.random.fold_in(splits[8], 1), 1, FAN_A).astype(jnp.int32)
    near_b = set_ends(jax.random.randint(splits[9], (SEEDS, FAN_B), 0, HOP_DEV), jax.random.fold_in(splits[9], 1), 0, HOP_DEV - 1).astype(jnp.int32)
    self_b = set_ends(jax.random.randint(splits[10], (SEEDS,), 0, HOP_DEV), jax.random.fold_in(splits[10], 1), 0, HOP_DEV - 1).astype(jnp.int32)
    count_b = set_ends(jax.random.randint(splits[11], (SEEDS,), 1, FAN_B + 1), jax.random.fold_in(splits[11], 1), 1, FAN_B).astype(jnp.int32)
    return {"table": table, "weight_a": weight_a, "bias_a": bias_a, "weight_b": weight_b, "bias_b": bias_b, "requests": requests, "near_a": near_a, "self_a": self_a, "count_a": count_a, "near_b": near_b, "self_b": self_b, "count_b": count_b}


def mean_rows(source, neighbours, counts):
    running = jnp.zeros((neighbours.shape[0], source.shape[1]), jnp.float32)
    for column in range(neighbours.shape[1]):
        keep_mask = (counts > column)[:, None]
        running = running + jnp.where(keep_mask, source[neighbours[:, column]].astype(jnp.float32), 0.0)
    return (running / counts[:, None].astype(jnp.float32)).astype(jnp.bfloat16)

def reference(table, weight_a, bias_a, weight_b, bias_b, requests, near_a, self_a, count_a, near_b, self_b, count_b):
    offsets = (jnp.arange(N_DOM) * NODE_DEV).astype(jnp.int32)[:, None]

    def per_device(blocks):
        asked, hop_near, hop_self, hop_count, seed_near, seed_self, seed_count = blocks
        row_ids = (asked + offsets).reshape(-1).astype(jnp.int32)
        fetched = table[row_ids]
        mean_a = mean_rows(fetched, hop_near, hop_count)
        inputs_a = jnp.concatenate([fetched[hop_self], mean_a], axis=1)
        before = jnp.dot(inputs_a, weight_a, preferred_element_type=jnp.float32) + bias_a
        hidden_a = jax.nn.relu(before).astype(jnp.bfloat16)
        mean_b = mean_rows(hidden_a, seed_near, seed_count)
        inputs_b = jnp.concatenate([hidden_a[seed_self], mean_b], axis=1)
        state = jax.nn.relu(jnp.dot(inputs_b, weight_b, preferred_element_type=jnp.float32) + bias_b)
        squares = lax.optimization_barrier(jnp.sum(state * state, axis=1, keepdims=True))
        return (state * jnp.sqrt(jnp.float32(H)) / jnp.sqrt(squares + H)).astype(jnp.bfloat16)
    blocks = (requests, near_a.reshape(N_DOM, HOP_DEV, FAN_A), self_a.reshape(N_DOM, HOP_DEV), count_a.reshape(N_DOM, HOP_DEV), near_b.reshape(N_DOM, SEEDS_DEV, FAN_B), self_b.reshape(N_DOM, SEEDS_DEV), count_b.reshape(N_DOM, SEEDS_DEV))
    result = lax.map(per_device, blocks)
    return result.reshape(N_DOM * SEEDS_DEV, H)
```

```python
import functools

import jax
import jax.numpy as jnp
from jax import lax
from jax.experimental import pallas as pl
from jax.experimental.pallas import tpu as pltpu
from jax.sharding import PartitionSpec as P

MESH = pl.DeviceIdType.MESH
VMEM = pl.BlockSpec(memory_space=pltpu.VMEM)
TILE = 256


def peer(me, step, n):
    return lax.rem(me + 1 + lax.rem(n // 2 - 1 + step, n - 1), n)


def greet(me, n, partner):
    barrier = pltpu.get_barrier_semaphore()

    def one(step, carry):
        pl.semaphore_signal(
            barrier, inc=1, device_id={"dom": peer(me, step, n)}, device_id_type=MESH
        )
        return carry

    lax.fori_loop(0, n - 1, one, 0)
    if partner is not None:
        pl.semaphore_signal(barrier, inc=1, device_id={"mp": partner}, device_id_type=MESH)
    pl.semaphore_wait(barrier, n - 1 + (partner is not None))


def block_copy(source, landed, me, other, send_sem, recv_sem):
    return pltpu.make_async_remote_copy(
        src_ref=source.at[other],
        dst_ref=landed.at[me],
        send_sem=send_sem.at[other],
        recv_sem=recv_sem.at[me],
        device_id={"dom": other},
        device_id_type=MESH,
    )


def send_blocks(source, landed, me, n, send_sem, recv_sem):
    def one(step, carry):
        block_copy(source, landed, me, peer(me, step, n), send_sem, recv_sem).start()
        return carry

    lax.fori_loop(0, n - 1, one, 0)


def finish_sends(source, landed, me, n, send_sem, recv_sem):
    def one(step, carry):
        block_copy(source, landed, me, peer(me, step, n), send_sem, recv_sem).wait_send()
        return carry

    lax.fori_loop(0, n - 1, one, 0)


def wait_block(source, landed, other, recv_sem):
    pltpu.make_async_copy(source.at[other], landed.at[other], recv_sem.at[other]).wait()


def ask_kernel(n, asked_ref, out_ref, landed, send_sem, recv_sem):
    me = lax.axis_index("dom")
    greet(me, n, None)
    send_blocks(asked_ref, landed, me, n, send_sem, recv_sem)
    pltpu.make_async_copy(asked_ref.at[me], landed.at[me], recv_sem.at[me]).start()

    def one(other, carry):
        wait_block(asked_ref, landed, other, recv_sem)
        return carry

    lax.fori_loop(0, n, one, 0)
    out_ref[...] = landed[...]
    finish_sends(asked_ref, landed, me, n, send_sem, recv_sem)


def ask(asked, n):
    return pl.pallas_call(
        functools.partial(ask_kernel, n),
        out_shape=jax.ShapeDtypeStruct(asked.shape, asked.dtype),
        in_specs=[VMEM],
        out_specs=VMEM,
        scratch_shapes=[
            pltpu.VMEM(asked.shape, asked.dtype),
            pltpu.SemaphoreType.DMA((n,)),
            pltpu.SemaphoreType.DMA((n,)),
        ],
        compiler_params=pltpu.CompilerParams(collective_id=0, has_side_effects=True),
        name="ask",
    )(asked)


def build_picks(index_ref, fan, mean_pick, own_pick):
    rows, columns = mean_pick.shape
    high, wide = 64, min(512, columns)

    def one(at, carry):
        r0 = pl.multiple_of(at // (columns // wide) * high, high)
        c0 = pl.multiple_of(at % (columns // wide) * wide, wide)
        index = index_ref[pl.ds(r0, high), :]
        column = lax.broadcasted_iota(jnp.int32, (high, wide), 1) + c0
        total = jnp.zeros((high, wide), jnp.float32)
        for j in range(fan):
            total = total + jnp.where(index[:, j : j + 1] == column, 1.0, 0.0)
        mean_pick[pl.ds(r0, high), pl.ds(c0, wide)] = total.astype(jnp.bfloat16)
        own = jnp.where(index[:, fan : fan + 1] == column, 1.0, 0.0)
        own_pick[pl.ds(r0, high), pl.ds(c0, wide)] = own.astype(jnp.bfloat16)
        return carry

    lax.fori_loop(0, rows // high * (columns // wide), one, 0)


def dot(a, b):
    return jnp.dot(a, b, preferred_element_type=jnp.float32)


def main_kernel(
    n, fan_a, fan_b,
    found_ref, index_a_ref, index_b_ref, weight_a_ref, bias_a_ref, weight_b_ref, bias_b_ref,
    out_ref,
    fetched, pick_a, self_pick_a, pick_b, self_pick_b, sum_mean, sum_own,
    mine_a, theirs_a, hidden, mine_b, theirs_b, mine_sq, theirs_sq,
    send_sem, recv_sem, mp_send, mp_recv,
):
    me = lax.axis_index("dom")
    core = lax.axis_index("mp")
    partner = 1 - core
    each, half = found_ref.shape[1], found_ref.shape[2]
    rows = sum_mean.shape[0]
    half_hidden = hidden.shape[1]
    feature, hidden_width = weight_a_ref.shape[0] // 2, weight_b_ref.shape[0] // 2
    seeds = out_ref.shape[0]

    greet(me, n, partner)
    send_blocks(found_ref, fetched, me, n, send_sem, recv_sem)
    pltpu.make_async_copy(found_ref.at[me], fetched.at[me], recv_sem.at[me]).start()
    build_picks(index_a_ref, fan_a, pick_a, self_pick_a)
    build_picks(index_b_ref, fan_b, pick_b, self_pick_b)
    sum_mean[...] = jnp.zeros_like(sum_mean)
    sum_own[...] = jnp.zeros_like(sum_own)

    per = min(n, max(1, 256 // each))
    groups = n // per
    depth = per * each

    def one_group(step, carry):
        group = lax.rem(me // per + step, groups)

        def arrive(i, inner):
            wait_block(found_ref, fetched, group * per + i, recv_sem)
            return inner

        lax.fori_loop(0, per, arrive, 0)
        columns = pl.ds(pl.multiple_of(group * depth, depth), depth)

        def one_tile(tile, inner):
            at = pl.ds(pl.multiple_of(tile * TILE, TILE), TILE)
            block = fetched[pl.ds(group * per, per)].reshape(depth, half)
            sum_mean[at, :] += dot(pick_a[at, columns], block)
            sum_own[at, :] += dot(self_pick_a[at, columns], block)
            return inner

        lax.fori_loop(0, rows // TILE, one_tile, 0)
        return carry

    lax.fori_loop(0, groups, one_group, 0)

    def swap(source, landed, at):
        return pltpu.make_async_remote_copy(
            src_ref=source,
            dst_ref=landed,
            send_sem=mp_send.at[at],
            recv_sem=mp_recv.at[at],
            device_id={"mp": partner},
            device_id_type=MESH,
        )

    mine_a[0] = sum_own[...].astype(jnp.bfloat16)
    count_a = index_a_ref[:, fan_a + 1 : fan_a + 2].astype(jnp.float32)
    mine_a[1] = (sum_mean[...] / count_a).astype(jnp.bfloat16)
    swap_a = swap(mine_a, theirs_a, 0)
    swap_a.start()

    def rows_of(weight_ref, start, width, which):
        return weight_ref[pl.ds(pl.multiple_of(start + which * width, 128), width), :]

    def layer_a(tile, carry):
        at = pl.ds(pl.multiple_of(tile * TILE, TILE), TILE)
        value = dot(mine_a[0, at, :], rows_of(weight_a_ref, 0, half, core))
        value = value + dot(mine_a[1, at, :], rows_of(weight_a_ref, feature, half, core))
        sum_own[at, pl.ds(0, half_hidden)] = value
        return carry

    def layer_a_rest(tile, carry):
        at = pl.ds(pl.multiple_of(tile * TILE, TILE), TILE)
        value = sum_own[at, pl.ds(0, half_hidden)]
        value = value + dot(theirs_a[0, at, :], rows_of(weight_a_ref, 0, half, partner))
        value = value + dot(theirs_a[1, at, :], rows_of(weight_a_ref, feature, half, partner))
        hidden[at, :] = jnp.maximum(value + bias_a_ref[...], 0.0).astype(jnp.bfloat16)
        return carry

    lax.fori_loop(0, rows // TILE, layer_a, 0)
    swap_a.wait()
    lax.fori_loop(0, rows // TILE, layer_a_rest, 0)

    mine_b[0] = dot(self_pick_b[...], hidden[...]).astype(jnp.bfloat16)
    count_b = index_b_ref[:, fan_b + 1 : fan_b + 2].astype(jnp.float32)
    mine_b[1] = (dot(pick_b[...], hidden[...]) / count_b).astype(jnp.bfloat16)
    swap_b = swap(mine_b, theirs_b, 1)
    swap_b.start()
    state = dot(mine_b[0], rows_of(weight_b_ref, 0, half_hidden, core))
    state = state + dot(mine_b[1], rows_of(weight_b_ref, hidden_width, half_hidden, core))
    swap_b.wait()
    state = state + dot(theirs_b[0], rows_of(weight_b_ref, 0, half_hidden, partner))
    state = state + dot(theirs_b[1], rows_of(weight_b_ref, hidden_width, half_hidden, partner))
    state = jnp.maximum(state + bias_b_ref[...], 0.0)
    mine_sq[...] = jnp.broadcast_to(jnp.sum(state * state, axis=1, keepdims=True), mine_sq.shape)
    swap_sq = swap(mine_sq, theirs_sq, 2)
    swap_sq.start()
    swap_sq.wait()
    squares = mine_sq[:, 0:1] + theirs_sq[:, 0:1]
    scale = jnp.sqrt(jnp.float32(hidden_width)) / jnp.sqrt(squares + hidden_width)
    out_ref[...] = (state * scale).astype(out_ref.dtype)
    finish_sends(found_ref, fetched, me, n, send_sem, recv_sem)


def main(n, fan_a, fan_b, found, index_a, index_b, weight_a, bias_a, weight_b, bias_b):
    slots = found.shape[0] * found.shape[1]
    half, rows, seeds = found.shape[2], index_a.shape[0], index_b.shape[0]
    half_hidden = weight_a.shape[1]
    bf16, f32 = jnp.bfloat16, jnp.float32
    return pl.pallas_call(
        functools.partial(main_kernel, n, fan_a, fan_b),
        out_shape=jax.ShapeDtypeStruct((seeds, half_hidden), bf16),
        in_specs=[VMEM] * 7,
        out_specs=VMEM,
        scratch_shapes=[
            pltpu.VMEM(found.shape, bf16),
            pltpu.VMEM((rows, slots), bf16),
            pltpu.VMEM((rows, slots), bf16),
            pltpu.VMEM((seeds, rows), bf16),
            pltpu.VMEM((seeds, rows), bf16),
            pltpu.VMEM((rows, half), f32),
            pltpu.VMEM((rows, half), f32),
            pltpu.VMEM((2, rows, half), bf16),
            pltpu.VMEM((2, rows, half), bf16),
            pltpu.VMEM((rows, half_hidden), bf16),
            pltpu.VMEM((2, seeds, half_hidden), bf16),
            pltpu.VMEM((2, seeds, half_hidden), bf16),
            pltpu.VMEM((seeds, 128), f32),
            pltpu.VMEM((seeds, 128), f32),
            pltpu.SemaphoreType.DMA((n,)),
            pltpu.SemaphoreType.DMA((n,)),
            pltpu.SemaphoreType.DMA((3,)),
            pltpu.SemaphoreType.DMA((3,)),
        ],
        compiler_params=pltpu.CompilerParams(collective_id=1, has_side_effects=True),
        name="sage",
    )(found, index_a, index_b, weight_a, bias_a, weight_b, bias_b)


def with_counts(near, own, count):
    fan = near.shape[1]
    column = lax.broadcasted_iota(jnp.int32, (1, fan), 1)
    kept = jnp.where(column < count[:, None], near, -1)
    return jnp.concatenate([kept, own[:, None], count[:, None]], axis=1)


def shards(
    n,
    table,
    weight_a,
    bias_a,
    weight_b,
    bias_b,
    requests,
    near_a,
    self_a,
    count_a,
    near_b,
    self_b,
    count_b,
):
    half_hidden = weight_a.shape[1]
    core = lax.axis_index("mp")
    asked = ask(requests[0][:, None, :], n)[:, 0, :]
    found = table[asked]
    bias_a = lax.dynamic_slice_in_dim(bias_a, core * half_hidden, half_hidden, 0)[None, :]
    bias_b = lax.dynamic_slice_in_dim(bias_b, core * half_hidden, half_hidden, 0)[None, :]
    index_a = with_counts(near_a, self_a, count_a)
    index_b = with_counts(near_b, self_b, count_b)
    return main(
        n, near_a.shape[1], near_b.shape[1],
        found, index_a, index_b, weight_a, bias_a, weight_b, bias_b,
    )


def solution(mesh):
    placed = (
        P("dom", "mp"),
        P(None, "mp"),
        P(),
        P(None, "mp"),
        P(),
        P("dom", None, None),
        P("dom", None),
        P("dom"),
        P("dom"),
        P("dom", None),
        P("dom"),
        P("dom"),
    )
    return jax.shard_map(
        functools.partial(shards, mesh.shape["dom"]),
        mesh=mesh, in_specs=placed, out_specs=P("dom", "mp"), check_vma=False,
    )
```

```python
import functools

import jax
import jax.numpy as jnp
from jax import lax
from jax.experimental import pallas as pl
from jax.experimental.pallas import tpu as pltpu
from jax.sharding import PartitionSpec as P

MESH = pl.DeviceIdType.MESH
VMEM = pl.BlockSpec(memory_space=pltpu.VMEM)
TILE = 256


def peer(me, step, n):
    return lax.rem(me + 1 + lax.rem(n // 2 - 1 + step, n - 1), n)


def greet(me, n, partner):
    barrier = pltpu.get_barrier_semaphore()

    def one(step, carry):
        pl.semaphore_signal(
            barrier, inc=1, device_id={"dom": peer(me, step, n)}, device_id_type=MESH
        )
        return carry

    lax.fori_loop(0, n - 1, one, 0)
    if partner is not None:
        pl.semaphore_signal(barrier, inc=1, device_id={"mp": partner}, device_id_type=MESH)
    pl.semaphore_wait(barrier, n - 1 + (partner is not None))


def block_copy(source, landed, me, other, send_sem, recv_sem):
    return pltpu.make_async_remote_copy(
        src_ref=source.at[other],
        dst_ref=landed.at[me],
        send_sem=send_sem.at[other],
        recv_sem=recv_sem.at[me],
        device_id={"dom": other},
        device_id_type=MESH,
    )


def send_blocks(source, landed, me, n, send_sem, recv_sem):
    def one(step, carry):
        block_copy(source, landed, me, peer(me, step, n), send_sem, recv_sem).start()
        return carry

    lax.fori_loop(0, n - 1, one, 0)


def finish_sends(source, landed, me, n, send_sem, recv_sem):
    def one(step, carry):
        block_copy(source, landed, me, peer(me, step, n), send_sem, recv_sem).wait_send()
        return carry

    lax.fori_loop(0, n - 1, one, 0)


def wait_block(source, landed, other, recv_sem):
    pltpu.make_async_copy(source.at[other], landed.at[other], recv_sem.at[other]).wait()


def build_picks(index_ref, fan, mean_pick, own_pick):
    rows, columns = mean_pick.shape
    high, wide = 64, min(512, columns)

    def one(at, carry):
        r0 = pl.multiple_of(at // (columns // wide) * high, high)
        c0 = pl.multiple_of(at % (columns // wide) * wide, wide)
        index = index_ref[pl.ds(r0, high), :]
        column = lax.broadcasted_iota(jnp.int32, (high, wide), 1) + c0
        total = jnp.zeros((high, wide), jnp.float32)
        for j in range(fan):
            total = total + jnp.where(index[:, j : j + 1] == column, 1.0, 0.0)
        mean_pick[pl.ds(r0, high), pl.ds(c0, wide)] = total.astype(jnp.bfloat16)
        own = jnp.where(index[:, fan : fan + 1] == column, 1.0, 0.0)
        own_pick[pl.ds(r0, high), pl.ds(c0, wide)] = own.astype(jnp.bfloat16)
        return carry

    lax.fori_loop(0, rows // high * (columns // wide), one, 0)


def dot(a, b):
    return jnp.dot(a, b, preferred_element_type=jnp.float32)


def index_rows(index, near_ref, own_ref, count_ref):
    fan, rows = near_ref.shape
    count = count_ref[...]
    pieces = [jnp.where(count > j, near_ref[j : j + 1, :], -1) for j in range(fan)]
    pieces += [own_ref[...], count, jnp.zeros((index.shape[1] - fan - 2, rows), jnp.int32)]
    index[...] = jnp.concatenate(pieces, axis=0).T


def main_kernel(
    n,
    asked_ref, table_ref, near_a_ref, self_a_ref, count_a_ref, near_b_ref, self_b_ref, count_b_ref,
    weight_a_any, bias_a_ref, weight_b_any, bias_b_ref,
    out_ref,
    table, table_wide, wanted, wanted_scalar, stage, found_ref,
    weight_a_ref, weight_b_ref, index_a_ref, index_b_ref,
    fetched, pick_a, self_pick_a, pick_b, self_pick_b, sum_mean, sum_own,
    mine_a, theirs_a, hidden, mine_b, theirs_b, mine_sq, theirs_sq,
    ask_send, ask_recv, send_sem, recv_sem, mp_send, mp_recv, load_sem,
):
    me = lax.axis_index("dom")
    core = lax.axis_index("mp")
    partner = 1 - core
    each, half = found_ref.shape[1], found_ref.shape[2]
    rows = sum_mean.shape[0]
    half_hidden = hidden.shape[1]
    feature, hidden_width = weight_a_ref.shape[0] // 2, weight_b_ref.shape[0] // 2
    fan_a, fan_b = near_a_ref.shape[0], near_b_ref.shape[0]

    load_table = pltpu.make_async_copy(table_ref, table, load_sem.at[0])
    load_table.start()
    greet(me, n, partner)
    send_blocks(asked_ref, wanted, me, n, ask_send, ask_recv)
    pltpu.make_async_copy(asked_ref.at[me], wanted.at[me], ask_recv.at[me]).start()
    load_table.wait()
    load_a = pltpu.make_async_copy(weight_a_any, weight_a_ref, load_sem.at[1])
    load_a.start()
    load_b = pltpu.make_async_copy(weight_b_any, weight_b_ref, load_sem.at[2])
    load_b.start()

    def widen(tile, carry):
        at = pl.ds(pl.multiple_of(tile * 128, 128), 128)
        table_wide[at, :] = table[at, :].astype(jnp.float32)
        return carry

    lax.fori_loop(0, table.shape[0] // 128, widen, 0)

    def asked_of(other, carry):
        wait_block(asked_ref, wanted, other, ask_recv)
        return carry

    lax.fori_loop(0, n, asked_of, 0)
    to_scalar = pltpu.make_async_copy(wanted, wanted_scalar, load_sem.at[3])
    to_scalar.start()
    to_scalar.wait()

    def find(other):
        def some(at, carry):
            r0 = at * 16
            for k in range(16):
                row = wanted_scalar[other, 0, r0 + k]
                stage[pl.ds(r0 + k, 1), :] = table_wide[pl.ds(row, 1), :]
            return carry

        lax.fori_loop(0, each // 16, some, 0)
        found_ref[other] = stage[...].astype(jnp.bfloat16)

    def find_and_send(step, carry):
        other = peer(me, step, n)
        find(other)
        block_copy(found_ref, fetched, me, other, send_sem, recv_sem).start()
        return carry

    lax.fori_loop(0, n - 1, find_and_send, 0)
    find(me)
    pltpu.make_async_copy(found_ref.at[me], fetched.at[me], recv_sem.at[me]).start()
    index_rows(index_a_ref, near_a_ref, self_a_ref, count_a_ref)
    index_rows(index_b_ref, near_b_ref, self_b_ref, count_b_ref)
    build_picks(index_a_ref, fan_a, pick_a, self_pick_a)
    build_picks(index_b_ref, fan_b, pick_b, self_pick_b)
    sum_mean[...] = jnp.zeros_like(sum_mean)
    sum_own[...] = jnp.zeros_like(sum_own)
    mine_cols = pl.ds(pl.multiple_of(core * half_hidden, 128), half_hidden)
    load_a.wait()
    load_b.wait()

    per = min(n, max(1, 256 // each))
    groups = n // per
    depth = per * each

    def one_group(step, carry):
        group = lax.rem(me // per + step, groups)

        def arrive(i, inner):
            wait_block(found_ref, fetched, group * per + i, recv_sem)
            return inner

        lax.fori_loop(0, per, arrive, 0)
        columns = pl.ds(pl.multiple_of(group * depth, depth), depth)

        def one_tile(tile, inner):
            at = pl.ds(pl.multiple_of(tile * TILE, TILE), TILE)
            block = fetched[pl.ds(group * per, per)].reshape(depth, half)
            sum_mean[at, :] += dot(pick_a[at, columns], block)
            sum_own[at, :] += dot(self_pick_a[at, columns], block)
            return inner

        lax.fori_loop(0, rows // TILE, one_tile, 0)
        return carry

    lax.fori_loop(0, groups, one_group, 0)

    def swap(source, landed, at):
        return pltpu.make_async_remote_copy(
            src_ref=source,
            dst_ref=landed,
            send_sem=mp_send.at[at],
            recv_sem=mp_recv.at[at],
            device_id={"mp": partner},
            device_id_type=MESH,
        )

    mine_a[0] = sum_own[...].astype(jnp.bfloat16)
    count_a = index_a_ref[:, fan_a + 1 : fan_a + 2].astype(jnp.float32)
    mine_a[1] = (sum_mean[...] / count_a).astype(jnp.bfloat16)
    swap_a = swap(mine_a, theirs_a, 0)
    swap_a.start()

    def rows_of(weight_ref, start, width, which):
        return weight_ref[pl.ds(pl.multiple_of(start + which * width, 128), width), :]

    def layer_a(tile, carry):
        at = pl.ds(pl.multiple_of(tile * TILE, TILE), TILE)
        value = dot(mine_a[0, at, :], rows_of(weight_a_ref, 0, half, core))
        value = value + dot(mine_a[1, at, :], rows_of(weight_a_ref, feature, half, core))
        sum_own[at, pl.ds(0, half_hidden)] = value
        return carry

    def layer_a_rest(tile, carry):
        at = pl.ds(pl.multiple_of(tile * TILE, TILE), TILE)
        value = sum_own[at, pl.ds(0, half_hidden)]
        value = value + dot(theirs_a[0, at, :], rows_of(weight_a_ref, 0, half, partner))
        value = value + dot(theirs_a[1, at, :], rows_of(weight_a_ref, feature, half, partner))
        hidden[at, :] = jnp.maximum(value + bias_a_ref[:, mine_cols], 0.0).astype(jnp.bfloat16)
        return carry

    lax.fori_loop(0, rows // TILE, layer_a, 0)
    swap_a.wait()
    lax.fori_loop(0, rows // TILE, layer_a_rest, 0)

    mine_b[0] = dot(self_pick_b[...], hidden[...]).astype(jnp.bfloat16)
    count_b = index_b_ref[:, fan_b + 1 : fan_b + 2].astype(jnp.float32)
    mine_b[1] = (dot(pick_b[...], hidden[...]) / count_b).astype(jnp.bfloat16)
    swap_b = swap(mine_b, theirs_b, 1)
    swap_b.start()
    state = dot(mine_b[0], rows_of(weight_b_ref, 0, half_hidden, core))
    state = state + dot(mine_b[1], rows_of(weight_b_ref, hidden_width, half_hidden, core))
    swap_b.wait()
    state = state + dot(theirs_b[0], rows_of(weight_b_ref, 0, half_hidden, partner))
    state = state + dot(theirs_b[1], rows_of(weight_b_ref, hidden_width, half_hidden, partner))
    state = jnp.maximum(state + bias_b_ref[:, mine_cols], 0.0)
    mine_sq[...] = jnp.broadcast_to(jnp.sum(state * state, axis=1, keepdims=True), mine_sq.shape)
    swap_sq = swap(mine_sq, theirs_sq, 2)
    swap_sq.start()
    swap_sq.wait()
    squares = mine_sq[:, 0:1] + theirs_sq[:, 0:1]
    scale = jnp.sqrt(jnp.float32(hidden_width)) / jnp.sqrt(squares + hidden_width)
    out_ref[...] = (state * scale).astype(out_ref.dtype)
    finish_sends(asked_ref, wanted, me, n, ask_send, ask_recv)
    finish_sends(found_ref, fetched, me, n, send_sem, recv_sem)


def shards(
    n,
    table,
    weight_a,
    bias_a,
    weight_b,
    bias_b,
    requests,
    near_a,
    self_a,
    count_a,
    near_b,
    self_b,
    count_b,
):
    each = requests.shape[2]
    half, half_hidden = table.shape[1], weight_a.shape[1]
    rows, seeds, slots = near_a.shape[0], near_b.shape[0], n * each
    wide = -(-(near_a.shape[1] + 2) // 8) * 8
    bf16, f32 = jnp.bfloat16, jnp.float32
    anywhere = pl.BlockSpec(memory_space=pl.ANY)
    return pl.pallas_call(
        functools.partial(main_kernel, n),
        out_shape=jax.ShapeDtypeStruct((seeds, half_hidden), bf16),
        in_specs=[VMEM, anywhere] + [VMEM] * 6 + [anywhere, VMEM, anywhere, VMEM],
        out_specs=VMEM,
        scratch_shapes=[
            pltpu.VMEM(table.shape, bf16),
            pltpu.VMEM(table.shape, f32),
            pltpu.VMEM((n, 1, each), jnp.int32),
            pltpu.SMEM((n, 1, each), jnp.int32),
            pltpu.VMEM((each, half), f32),
            pltpu.VMEM((n, each, half), bf16),
            pltpu.VMEM(weight_a.shape, bf16),
            pltpu.VMEM(weight_b.shape, bf16),
            pltpu.VMEM((rows, wide), jnp.int32),
            pltpu.VMEM((seeds, wide), jnp.int32),
            pltpu.VMEM((n, each, half), bf16),
            pltpu.VMEM((rows, slots), bf16),
            pltpu.VMEM((rows, slots), bf16),
            pltpu.VMEM((seeds, rows), bf16),
            pltpu.VMEM((seeds, rows), bf16),
            pltpu.VMEM((rows, half), f32),
            pltpu.VMEM((rows, half), f32),
            pltpu.VMEM((2, rows, half), bf16),
            pltpu.VMEM((2, rows, half), bf16),
            pltpu.VMEM((rows, half_hidden), bf16),
            pltpu.VMEM((2, seeds, half_hidden), bf16),
            pltpu.VMEM((2, seeds, half_hidden), bf16),
            pltpu.VMEM((seeds, 128), f32),
            pltpu.VMEM((seeds, 128), f32),
            pltpu.SemaphoreType.DMA((n,)),
            pltpu.SemaphoreType.DMA((n,)),
            pltpu.SemaphoreType.DMA((n,)),
            pltpu.SemaphoreType.DMA((n,)),
            pltpu.SemaphoreType.DMA((3,)),
            pltpu.SemaphoreType.DMA((3,)),
            pltpu.SemaphoreType.DMA((4,)),
        ],
        compiler_params=pltpu.CompilerParams(
            collective_id=0, has_side_effects=True, vmem_limit_bytes=60 * 1024 * 1024
        ),
        name="sage",
    )(
        requests[0][:, None, :], table,
        near_a.T, self_a[None, :], count_a[None, :], near_b.T, self_b[None, :], count_b[None, :],
        weight_a, bias_a[None, :], weight_b, bias_b[None, :],
    )


def solution(mesh):
    placed = (
        P("dom", "mp"),
        P(None, "mp"),
        P(),
        P(None, "mp"),
        P(),
        P("dom", None, None),
        P("dom", None),
        P("dom"),
        P("dom"),
        P("dom", None),
        P("dom"),
        P("dom"),
    )
    return jax.shard_map(
        functools.partial(shards, mesh.shape["dom"]),
        mesh=mesh, in_specs=placed, out_specs=P("dom", "mp"), check_vma=False,
    )
```

```python
import functools

import jax
import jax.numpy as jnp
from jax import lax
from jax.experimental import pallas as pl
from jax.experimental.pallas import tpu as pltpu
from jax.sharding import PartitionSpec as P

MESH = pl.DeviceIdType.MESH
VMEM = pl.BlockSpec(memory_space=pltpu.VMEM)
TILE = 256


def peer(me, step, n):
    if n & (n - 1):
        return lax.rem(me + 1 + lax.rem(n // 2 - 1 + step, n - 1), n)
    other, mask, bit = 0, n - 1 - step, 1
    while bit < n:
        other = other + lax.rem(me // bit + mask // bit, 2) * bit
        bit *= 2
    return other


def greet(me, n, partner):
    barrier = pltpu.get_barrier_semaphore()

    def one(step, carry):
        pl.semaphore_signal(
            barrier, inc=1, device_id={"dom": peer(me, step, n)}, device_id_type=MESH
        )
        return carry

    lax.fori_loop(0, n - 1, one, 0)
    if partner is not None:
        pl.semaphore_signal(barrier, inc=1, device_id={"mp": partner}, device_id_type=MESH)
    pl.semaphore_wait(barrier, n - 1 + (partner is not None))


def block_copy(source, landed, me, other, send_sem, recv_sem):
    return pltpu.make_async_remote_copy(
        src_ref=source.at[other],
        dst_ref=landed.at[me],
        send_sem=send_sem.at[other],
        recv_sem=recv_sem.at[me],
        device_id={"dom": other},
        device_id_type=MESH,
    )


def send_blocks(source, landed, me, n, send_sem, recv_sem):
    def one(step, carry):
        block_copy(source, landed, me, peer(me, step, n), send_sem, recv_sem).start()
        return carry

    lax.fori_loop(0, n - 1, one, 0)


def finish_sends(source, landed, me, n, send_sem, recv_sem):
    def one(step, carry):
        block_copy(source, landed, me, peer(me, step, n), send_sem, recv_sem).wait_send()
        return carry

    lax.fori_loop(0, n - 1, one, 0)


def wait_block(source, landed, other, recv_sem):
    pltpu.make_async_copy(source.at[other], landed.at[other], recv_sem.at[other]).wait()


def build_picks(index_ref, fan, mean_pick, own_pick):
    rows, columns = mean_pick.shape
    high = 16
    short = jnp.int16 if columns < 2**15 else jnp.int32

    def one(at, carry):
        r0 = pl.multiple_of(at * high, high)
        index = index_ref[pl.ds(r0, high), :]
        lanes = [
            jnp.broadcast_to(index[:, j : j + 1], (high, 128)).astype(short)
            for j in range(fan + 1)
        ]
        lane = lax.broadcasted_iota(jnp.int32, (high, 128), 1)
        one_value, no_value = jnp.bfloat16(1.0), jnp.bfloat16(0.0)
        for c in range(0, columns, 128):
            column = (lane + c).astype(short)
            total = jnp.where(lanes[0] == column, one_value, no_value)
            for j in range(1, fan):
                total = total + jnp.where(lanes[j] == column, one_value, no_value)
            mean_pick[pl.ds(r0, high), c : c + 128] = total
            own_pick[pl.ds(r0, high), c : c + 128] = jnp.where(
                lanes[fan] == column, one_value, no_value
            )
        return carry

    lax.fori_loop(0, rows // high, one, 0)


def dot(a, b):
    return jnp.dot(a, b, preferred_element_type=jnp.float32)


def index_rows(index, near_ref, own_ref, count_ref):
    fan, rows = near_ref.shape
    count = count_ref[...]
    pieces = [jnp.where(count > j, near_ref[j : j + 1, :], -1) for j in range(fan)]
    pieces += [own_ref[...], count, jnp.zeros((index.shape[1] - fan - 2, rows), jnp.int32)]
    index[...] = jnp.concatenate(pieces, axis=0).T


def main_kernel(
    n,
    asked_ref, table_ref, near_a_ref, self_a_ref, count_a_ref, near_b_ref, self_b_ref, count_b_ref,
    weight_a_any, bias_a_ref, weight_b_any, bias_b_ref,
    out_ref,
    table, table_wide, wanted, wanted_scalar, stage, found_ref,
    weight_a_ref, weight_b_ref, index_a_ref, index_b_ref,
    fetched, pick_a, self_pick_a, pick_b, self_pick_b, sum_mean, sum_own,
    mine_a, theirs_a, hidden, mine_b, theirs_b, mine_sq, theirs_sq,
    ask_send, ask_recv, send_sem, recv_sem, mp_send, mp_recv, load_sem, scalar_sem,
):
    me = lax.axis_index("dom")
    core = lax.axis_index("mp")
    partner = 1 - core
    each, half = found_ref.shape[1], found_ref.shape[2]
    rows = sum_mean.shape[0]
    half_hidden = hidden.shape[1]
    feature, hidden_width = weight_a_ref.shape[0] // 2, weight_b_ref.shape[0] // 2
    fan_a, fan_b = near_a_ref.shape[0], near_b_ref.shape[0]

    load_table = pltpu.make_async_copy(table_ref, table, load_sem.at[0])
    load_table.start()
    greet(me, n, partner)
    send_blocks(asked_ref, wanted, me, n, ask_send, ask_recv)
    pltpu.make_async_copy(asked_ref.at[me], wanted.at[me], ask_recv.at[me]).start()
    load_table.wait()
    load_a = pltpu.make_async_copy(weight_a_any, weight_a_ref, load_sem.at[1])
    load_a.start()
    load_b = pltpu.make_async_copy(weight_b_any, weight_b_ref, load_sem.at[2])
    load_b.start()

    def widen(tile, carry):
        at = pl.ds(pl.multiple_of(tile * 128, 128), 128)
        table_wide[at, :] = table[at, :].astype(jnp.float32)
        return carry

    lax.fori_loop(0, table.shape[0] // 128, widen, 0)
    index_rows(index_a_ref, near_a_ref, self_a_ref, count_a_ref)
    index_rows(index_b_ref, near_b_ref, self_b_ref, count_b_ref)

    def to_scalar(other):
        return pltpu.make_async_copy(wanted.at[other], wanted_scalar.at[other], scalar_sem.at[other])

    def asked_of(step, carry):
        other = peer(me, step, n)
        wait_block(asked_ref, wanted, other, ask_recv)
        to_scalar(other).start()
        return carry

    lax.fori_loop(0, n - 1, asked_of, 0)
    wait_block(asked_ref, wanted, me, ask_recv)
    to_scalar(me).start()

    def find(other):
        to_scalar(other).wait()

        def some(at, carry):
            r0 = at * 16
            for k in range(16):
                row = wanted_scalar[other, 0, r0 + k]
                stage[pl.ds(r0 + k, 1), :] = table_wide[pl.ds(row, 1), :]
            return carry

        lax.fori_loop(0, each // 16, some, 0)
        found_ref[other] = stage[...].astype(jnp.bfloat16)

    def find_and_send(step, carry):
        other = peer(me, step, n)
        find(other)
        block_copy(found_ref, fetched, me, other, send_sem, recv_sem).start()
        return carry

    lax.fori_loop(0, n - 1, find_and_send, 0)
    find(me)
    pltpu.make_async_copy(found_ref.at[me], fetched.at[me], recv_sem.at[me]).start()
    build_picks(index_a_ref, fan_a, pick_a, self_pick_a)
    build_picks(index_b_ref, fan_b, pick_b, self_pick_b)
    sum_mean[...] = jnp.zeros_like(sum_mean)
    sum_own[...] = jnp.zeros_like(sum_own)
    mine_cols = pl.ds(pl.multiple_of(core * half_hidden, 128), half_hidden)
    load_a.wait()
    load_b.wait()

    per = min(n, max(1, 256 // each))
    groups = n // per
    depth = per * each

    def one_group(step, carry):
        group = lax.rem(me // per + step, groups)

        def arrive(i, inner):
            wait_block(found_ref, fetched, group * per + i, recv_sem)
            return inner

        lax.fori_loop(0, per, arrive, 0)
        columns = pl.ds(pl.multiple_of(group * depth, depth), depth)

        def one_tile(tile, inner):
            at = pl.ds(pl.multiple_of(tile * TILE, TILE), TILE)
            block = fetched[pl.ds(group * per, per)].reshape(depth, half)
            sum_mean[at, :] += dot(pick_a[at, columns], block)
            sum_own[at, :] += dot(self_pick_a[at, columns], block)
            return inner

        lax.fori_loop(0, rows // TILE, one_tile, 0)
        return carry

    lax.fori_loop(0, groups, one_group, 0)

    def swap(source, landed, at):
        return pltpu.make_async_remote_copy(
            src_ref=source,
            dst_ref=landed,
            send_sem=mp_send.at[at],
            recv_sem=mp_recv.at[at],
            device_id={"mp": partner},
            device_id_type=MESH,
        )

    def rows_of(weight_ref, start, width, which):
        return weight_ref[pl.ds(pl.multiple_of(start + which * width, 128), width), :]

    def swap_a(tile):
        return swap(mine_a.at[tile], theirs_a.at[tile], 2 + tile)

    def layer_a(tile, carry):
        at = pl.ds(pl.multiple_of(tile * TILE, TILE), TILE)
        count = index_a_ref[at, fan_a + 1 : fan_a + 2].astype(jnp.float32)
        mine_a[tile, 0] = sum_own[at, :].astype(jnp.bfloat16)
        mine_a[tile, 1] = (sum_mean[at, :] / count).astype(jnp.bfloat16)
        swap_a(tile).start()
        value = dot(mine_a[tile, 0], rows_of(weight_a_ref, 0, half, core))
        value = value + dot(mine_a[tile, 1], rows_of(weight_a_ref, feature, half, core))
        sum_own[at, pl.ds(0, half_hidden)] = value
        return carry

    def layer_a_rest(tile, carry):
        at = pl.ds(pl.multiple_of(tile * TILE, TILE), TILE)
        swap_a(tile).wait()
        value = sum_own[at, pl.ds(0, half_hidden)]
        value = value + dot(theirs_a[tile, 0], rows_of(weight_a_ref, 0, half, partner))
        value = value + dot(theirs_a[tile, 1], rows_of(weight_a_ref, feature, half, partner))
        hidden[at, :] = jnp.maximum(value + bias_a_ref[:, mine_cols], 0.0).astype(jnp.bfloat16)
        return carry

    lax.fori_loop(0, rows // TILE, layer_a, 0)
    lax.fori_loop(0, rows // TILE, layer_a_rest, 0)

    mine_b[0] = dot(self_pick_b[...], hidden[...]).astype(jnp.bfloat16)
    count_b = index_b_ref[:, fan_b + 1 : fan_b + 2].astype(jnp.float32)
    mine_b[1] = (dot(pick_b[...], hidden[...]) / count_b).astype(jnp.bfloat16)
    swap_b = swap(mine_b, theirs_b, 0)
    swap_b.start()
    state = dot(mine_b[0], rows_of(weight_b_ref, 0, half_hidden, core))
    state = state + dot(mine_b[1], rows_of(weight_b_ref, hidden_width, half_hidden, core))
    swap_b.wait()
    state = state + dot(theirs_b[0], rows_of(weight_b_ref, 0, half_hidden, partner))
    state = state + dot(theirs_b[1], rows_of(weight_b_ref, hidden_width, half_hidden, partner))
    state = jnp.maximum(state + bias_b_ref[:, mine_cols], 0.0)
    mine_sq[...] = jnp.broadcast_to(jnp.sum(state * state, axis=1, keepdims=True), mine_sq.shape)
    swap_sq = swap(mine_sq, theirs_sq, 1)
    swap_sq.start()
    swap_sq.wait()
    squares = mine_sq[:, 0:1] + theirs_sq[:, 0:1]
    scale = jnp.sqrt(jnp.float32(hidden_width)) / jnp.sqrt(squares + hidden_width)
    out_ref[...] = (state * scale).astype(out_ref.dtype)
    finish_sends(asked_ref, wanted, me, n, ask_send, ask_recv)
    finish_sends(found_ref, fetched, me, n, send_sem, recv_sem)


def shards(
    n,
    table,
    weight_a,
    bias_a,
    weight_b,
    bias_b,
    requests,
    near_a,
    self_a,
    count_a,
    near_b,
    self_b,
    count_b,
):
    each = requests.shape[2]
    half, half_hidden = table.shape[1], weight_a.shape[1]
    rows, seeds, slots = near_a.shape[0], near_b.shape[0], n * each
    wide = -(-(near_a.shape[1] + 2) // 8) * 8
    bf16, f32 = jnp.bfloat16, jnp.float32
    anywhere = pl.BlockSpec(memory_space=pl.ANY)
    return pl.pallas_call(
        functools.partial(main_kernel, n),
        out_shape=jax.ShapeDtypeStruct((seeds, half_hidden), bf16),
        in_specs=[VMEM, anywhere] + [VMEM] * 6 + [anywhere, VMEM, anywhere, VMEM],
        out_specs=VMEM,
        scratch_shapes=[
            pltpu.VMEM(table.shape, bf16),
            pltpu.VMEM(table.shape, f32),
            pltpu.VMEM((n, 1, each), jnp.int32),
            pltpu.SMEM((n, 1, each), jnp.int32),
            pltpu.VMEM((each, half), f32),
            pltpu.VMEM((n, each, half), bf16),
            pltpu.VMEM(weight_a.shape, bf16),
            pltpu.VMEM(weight_b.shape, bf16),
            pltpu.VMEM((rows, wide), jnp.int32),
            pltpu.VMEM((seeds, wide), jnp.int32),
            pltpu.VMEM((n, each, half), bf16),
            pltpu.VMEM((rows, slots), bf16),
            pltpu.VMEM((rows, slots), bf16),
            pltpu.VMEM((seeds, rows), bf16),
            pltpu.VMEM((seeds, rows), bf16),
            pltpu.VMEM((rows, half), f32),
            pltpu.VMEM((rows, half), f32),
            pltpu.VMEM((rows // TILE, 2, TILE, half), bf16),
            pltpu.VMEM((rows // TILE, 2, TILE, half), bf16),
            pltpu.VMEM((rows, half_hidden), bf16),
            pltpu.VMEM((2, seeds, half_hidden), bf16),
            pltpu.VMEM((2, seeds, half_hidden), bf16),
            pltpu.VMEM((seeds, 128), f32),
            pltpu.VMEM((seeds, 128), f32),
            pltpu.SemaphoreType.DMA((n,)),
            pltpu.SemaphoreType.DMA((n,)),
            pltpu.SemaphoreType.DMA((n,)),
            pltpu.SemaphoreType.DMA((n,)),
            pltpu.SemaphoreType.DMA((2 + rows // TILE,)),
            pltpu.SemaphoreType.DMA((2 + rows // TILE,)),
            pltpu.SemaphoreType.DMA((3,)),
            pltpu.SemaphoreType.DMA((n,)),
        ],
        compiler_params=pltpu.CompilerParams(
            collective_id=0, has_side_effects=True, vmem_limit_bytes=60 * 1024 * 1024
        ),
        name="sage",
    )(
        requests[0][:, None, :], table,
        near_a.T, self_a[None, :], count_a[None, :], near_b.T, self_b[None, :], count_b[None, :],
        weight_a, bias_a[None, :], weight_b, bias_b[None, :],
    )


def solution(mesh):
    placed = (
        P("dom", "mp"),
        P(None, "mp"),
        P(),
        P(None, "mp"),
        P(),
        P("dom", None, None),
        P("dom", None),
        P("dom"),
        P("dom"),
        P("dom", None),
        P("dom"),
        P("dom"),
    )
    return jax.shard_map(
        functools.partial(shards, mesh.shape["dom"]),
        mesh=mesh, in_specs=placed, out_specs=P("dom", "mp"), check_vma=False,
    )
```

```python
import functools

import jax
import jax.numpy as jnp
from jax import lax
from jax.experimental import pallas as pl
from jax.experimental.pallas import tpu as pltpu
from jax.sharding import PartitionSpec as P

MESH = pl.DeviceIdType.MESH
VMEM = pl.BlockSpec(memory_space=pltpu.VMEM)
TILE = 256


def peer(me, step, n):
    if n & (n - 1):
        return lax.rem(me + 1 + lax.rem(n // 2 - 1 + step, n - 1), n)
    return exchanged(me, n - 1 - step, n)


def exchanged(me, mask, n):
    other, bit = 0, 1
    while bit < n:
        other = other + lax.rem(me // bit + mask // bit, 2) * bit
        bit *= 2
    return other


def greet(me, n, partner):
    barrier = pltpu.get_barrier_semaphore()

    def one(step, carry):
        pl.semaphore_signal(
            barrier, inc=1, device_id={"dom": peer(me, step, n)}, device_id_type=MESH
        )
        return carry

    lax.fori_loop(0, n - 1, one, 0)
    if partner is not None:
        pl.semaphore_signal(barrier, inc=1, device_id={"mp": partner}, device_id_type=MESH)
    pl.semaphore_wait(barrier, n - 1 + (partner is not None))


def block_copy(source, landed, me, other, send_sem, recv_sem):
    return pltpu.make_async_remote_copy(
        src_ref=source.at[other],
        dst_ref=landed.at[me],
        send_sem=send_sem.at[other],
        recv_sem=recv_sem.at[me],
        device_id={"dom": other},
        device_id_type=MESH,
    )


def send_blocks(source, landed, me, n, send_sem, recv_sem):
    def one(step, carry):
        block_copy(source, landed, me, peer(me, step, n), send_sem, recv_sem).start()
        return carry

    lax.fori_loop(0, n - 1, one, 0)


def finish_sends(source, landed, me, n, send_sem, recv_sem):
    def one(step, carry):
        block_copy(source, landed, me, peer(me, step, n), send_sem, recv_sem).wait_send()
        return carry

    lax.fori_loop(0, n - 1, one, 0)


def wait_block(source, landed, other, recv_sem):
    pltpu.make_async_copy(source.at[other], landed.at[other], recv_sem.at[other]).wait()


def build_picks(index_ref, fan, mean_pick, own_pick):
    rows, columns = mean_pick.shape
    high = 16
    short = jnp.int16 if columns < 2**15 else jnp.int32

    def one(at, carry):
        r0 = pl.multiple_of(at * high, high)
        index = index_ref[pl.ds(r0, high), :]
        lanes = [
            jnp.broadcast_to(index[:, j : j + 1], (high, 128)).astype(short)
            for j in range(fan + 1)
        ]
        lane = lax.broadcasted_iota(jnp.int32, (high, 128), 1)
        one_value, no_value = jnp.bfloat16(1.0), jnp.bfloat16(0.0)
        for c in range(0, columns, 128):
            column = (lane + c).astype(short)
            total = jnp.where(lanes[0] == column, one_value, no_value)
            for j in range(1, fan):
                total = total + jnp.where(lanes[j] == column, one_value, no_value)
            mean_pick[pl.ds(r0, high), c : c + 128] = total
            own_pick[pl.ds(r0, high), c : c + 128] = jnp.where(
                lanes[fan] == column, one_value, no_value
            )
        return carry

    lax.fori_loop(0, rows // high, one, 0)


def dot(a, b):
    return jnp.dot(a, b, preferred_element_type=jnp.float32)


def index_rows(index, near_ref, own_ref, count_ref):
    fan, rows = near_ref.shape
    count = count_ref[...]
    pieces = [jnp.where(count > j, near_ref[j : j + 1, :], -1) for j in range(fan)]
    pieces += [own_ref[...], count, jnp.zeros((index.shape[1] - fan - 2, rows), jnp.int32)]
    index[...] = jnp.concatenate(pieces, axis=0).T


def main_kernel(
    n,
    asked_ref, table_ref, near_a_ref, self_a_ref, count_a_ref, near_b_ref, self_b_ref, count_b_ref,
    weight_a_any, bias_a_ref, weight_b_any, bias_b_ref,
    out_ref,
    table, table_wide, wanted, wanted_scalar, stage, found_ref,
    weight_a_ref, weight_b_ref, index_a_ref, index_b_ref,
    fetched, pick_a, self_pick_a, pick_b, self_pick_b, sum_mean, sum_own,
    mine_a, theirs_a, hidden, mine_b, theirs_b, mine_sq, theirs_sq,
    ask_send, ask_recv, send_sem, recv_sem, mp_send, mp_recv, load_sem, scalar_sem,
):
    me = lax.axis_index("dom")
    core = lax.axis_index("mp")
    partner = 1 - core
    each, half = found_ref.shape[1], found_ref.shape[2]
    rows = sum_mean.shape[0]
    half_hidden = hidden.shape[1]
    feature, hidden_width = weight_a_ref.shape[0] // 2, weight_b_ref.shape[0] // 2
    fan_a, fan_b = near_a_ref.shape[0], near_b_ref.shape[0]

    load_table = pltpu.make_async_copy(table_ref, table, load_sem.at[0])
    load_table.start()
    greet(me, n, partner)
    send_blocks(asked_ref, wanted, me, n, ask_send, ask_recv)
    pltpu.make_async_copy(asked_ref.at[me], wanted.at[me], ask_recv.at[me]).start()
    load_table.wait()
    load_a = pltpu.make_async_copy(weight_a_any, weight_a_ref, load_sem.at[1])
    load_a.start()
    load_b = pltpu.make_async_copy(weight_b_any, weight_b_ref, load_sem.at[2])
    load_b.start()

    def widen(tile, carry):
        at = pl.ds(pl.multiple_of(tile * 128, 128), 128)
        table_wide[at, :] = table[at, :].astype(jnp.float32)
        return carry

    lax.fori_loop(0, table.shape[0] // 128, widen, 0)
    index_rows(index_a_ref, near_a_ref, self_a_ref, count_a_ref)
    index_rows(index_b_ref, near_b_ref, self_b_ref, count_b_ref)

    def to_scalar(other):
        return pltpu.make_async_copy(wanted.at[other], wanted_scalar.at[other], scalar_sem.at[other])

    def find(other):
        to_scalar(other).wait()

        def some(at, carry):
            r0 = at * 16
            for k in range(16):
                row = wanted_scalar[other, 0, r0 + k]
                stage[pl.ds(r0 + k, 1), :] = table_wide[pl.ds(row, 1), :]
            return carry

        lax.fori_loop(0, each // 16, some, 0)
        found_ref[other] = stage[...].astype(jnp.bfloat16)

    behind = min(2, n - 1)

    def asked_of(step):
        other = peer(me, step, n)
        wait_block(asked_ref, wanted, other, ask_recv)
        to_scalar(other).start()

    def find_and_send(step, carry):
        @pl.when(step < n - 1)
        def _():
            asked_of(step)

        @pl.when(step >= behind)
        def _():
            other = peer(me, step - behind, n)
            find(other)
            block_copy(found_ref, fetched, me, other, send_sem, recv_sem).start()

        return carry

    lax.fori_loop(0, n - 1 + behind, find_and_send, 0)
    wait_block(asked_ref, wanted, me, ask_recv)
    to_scalar(me).start()
    find(me)
    pltpu.make_async_copy(found_ref.at[me], fetched.at[me], recv_sem.at[me]).start()
    build_picks(index_a_ref, fan_a, pick_a, self_pick_a)
    build_picks(index_b_ref, fan_b, pick_b, self_pick_b)
    sum_mean[...] = jnp.zeros_like(sum_mean)
    sum_own[...] = jnp.zeros_like(sum_own)
    mine_cols = pl.ds(pl.multiple_of(core * half_hidden, 128), half_hidden)
    load_a.wait()
    load_b.wait()

    per = min(n, max(1, 256 // each))
    groups = n // per
    depth = per * each

    def one_group(step, carry):
        group = exchanged(me // per, lax.rem(groups - step, groups), groups)

        def arrive(i, inner):
            wait_block(found_ref, fetched, group * per + i, recv_sem)
            return inner

        lax.fori_loop(0, per, arrive, 0)
        columns = pl.ds(pl.multiple_of(group * depth, depth), depth)

        def one_tile(tile, inner):
            at = pl.ds(pl.multiple_of(tile * TILE, TILE), TILE)
            block = fetched[pl.ds(group * per, per)].reshape(depth, half)
            sum_mean[at, :] += dot(pick_a[at, columns], block)
            sum_own[at, :] += dot(self_pick_a[at, columns], block)
            return inner

        lax.fori_loop(0, rows // TILE, one_tile, 0)
        return carry

    lax.fori_loop(0, groups, one_group, 0)

    def swap(source, landed, at):
        return pltpu.make_async_remote_copy(
            src_ref=source,
            dst_ref=landed,
            send_sem=mp_send.at[at],
            recv_sem=mp_recv.at[at],
            device_id={"mp": partner},
            device_id_type=MESH,
        )

    def rows_of(weight_ref, start, width, which):
        return weight_ref[pl.ds(pl.multiple_of(start + which * width, 128), width), :]

    def swap_a(tile):
        return swap(mine_a.at[tile], theirs_a.at[tile], 2 + tile)

    def layer_a(tile, carry):
        at = pl.ds(pl.multiple_of(tile * TILE, TILE), TILE)
        count = index_a_ref[at, fan_a + 1 : fan_a + 2].astype(jnp.float32)
        mine_a[tile, 0] = sum_own[at, :].astype(jnp.bfloat16)
        mine_a[tile, 1] = (sum_mean[at, :] / count).astype(jnp.bfloat16)
        swap_a(tile).start()
        value = dot(mine_a[tile, 0], rows_of(weight_a_ref, 0, half, core))
        value = value + dot(mine_a[tile, 1], rows_of(weight_a_ref, feature, half, core))
        sum_own[at, pl.ds(0, half_hidden)] = value
        return carry

    def layer_a_rest(tile, carry):
        at = pl.ds(pl.multiple_of(tile * TILE, TILE), TILE)
        swap_a(tile).wait()
        value = sum_own[at, pl.ds(0, half_hidden)]
        value = value + dot(theirs_a[tile, 0], rows_of(weight_a_ref, 0, half, partner))
        value = value + dot(theirs_a[tile, 1], rows_of(weight_a_ref, feature, half, partner))
        hidden[at, :] = jnp.maximum(value + bias_a_ref[:, mine_cols], 0.0).astype(jnp.bfloat16)
        return carry

    lax.fori_loop(0, rows // TILE, layer_a, 0)
    lax.fori_loop(0, rows // TILE, layer_a_rest, 0)

    mine_b[0] = dot(self_pick_b[...], hidden[...]).astype(jnp.bfloat16)
    count_b = index_b_ref[:, fan_b + 1 : fan_b + 2].astype(jnp.float32)
    mine_b[1] = (dot(pick_b[...], hidden[...]) / count_b).astype(jnp.bfloat16)
    swap_b = swap(mine_b, theirs_b, 0)
    swap_b.start()
    state = dot(mine_b[0], rows_of(weight_b_ref, 0, half_hidden, core))
    state = state + dot(mine_b[1], rows_of(weight_b_ref, hidden_width, half_hidden, core))
    swap_b.wait()
    state = state + dot(theirs_b[0], rows_of(weight_b_ref, 0, half_hidden, partner))
    state = state + dot(theirs_b[1], rows_of(weight_b_ref, hidden_width, half_hidden, partner))
    state = jnp.maximum(state + bias_b_ref[:, mine_cols], 0.0)
    mine_sq[...] = jnp.broadcast_to(jnp.sum(state * state, axis=1, keepdims=True), mine_sq.shape)
    swap_sq = swap(mine_sq, theirs_sq, 1)
    swap_sq.start()
    swap_sq.wait()
    squares = mine_sq[:, 0:1] + theirs_sq[:, 0:1]
    scale = jnp.sqrt(jnp.float32(hidden_width)) / jnp.sqrt(squares + hidden_width)
    out_ref[...] = (state * scale).astype(out_ref.dtype)
    finish_sends(asked_ref, wanted, me, n, ask_send, ask_recv)
    finish_sends(found_ref, fetched, me, n, send_sem, recv_sem)


def shards(
    n,
    table,
    weight_a,
    bias_a,
    weight_b,
    bias_b,
    requests,
    near_a,
    self_a,
    count_a,
    near_b,
    self_b,
    count_b,
):
    each = requests.shape[2]
    half, half_hidden = table.shape[1], weight_a.shape[1]
    rows, seeds, slots = near_a.shape[0], near_b.shape[0], n * each
    wide = -(-(near_a.shape[1] + 2) // 8) * 8
    bf16, f32 = jnp.bfloat16, jnp.float32
    anywhere = pl.BlockSpec(memory_space=pl.ANY)
    return pl.pallas_call(
        functools.partial(main_kernel, n),
        out_shape=jax.ShapeDtypeStruct((seeds, half_hidden), bf16),
        in_specs=[VMEM, anywhere] + [VMEM] * 6 + [anywhere, VMEM, anywhere, VMEM],
        out_specs=VMEM,
        scratch_shapes=[
            pltpu.VMEM(table.shape, bf16),
            pltpu.VMEM(table.shape, f32),
            pltpu.VMEM((n, 1, each), jnp.int32),
            pltpu.SMEM((n, 1, each), jnp.int32),
            pltpu.VMEM((each, half), f32),
            pltpu.VMEM((n, each, half), bf16),
            pltpu.VMEM(weight_a.shape, bf16),
            pltpu.VMEM(weight_b.shape, bf16),
            pltpu.VMEM((rows, wide), jnp.int32),
            pltpu.VMEM((seeds, wide), jnp.int32),
            pltpu.VMEM((n, each, half), bf16),
            pltpu.VMEM((rows, slots), bf16),
            pltpu.VMEM((rows, slots), bf16),
            pltpu.VMEM((seeds, rows), bf16),
            pltpu.VMEM((seeds, rows), bf16),
            pltpu.VMEM((rows, half), f32),
            pltpu.VMEM((rows, half), f32),
            pltpu.VMEM((rows // TILE, 2, TILE, half), bf16),
            pltpu.VMEM((rows // TILE, 2, TILE, half), bf16),
            pltpu.VMEM((rows, half_hidden), bf16),
            pltpu.VMEM((2, seeds, half_hidden), bf16),
            pltpu.VMEM((2, seeds, half_hidden), bf16),
            pltpu.VMEM((seeds, 128), f32),
            pltpu.VMEM((seeds, 128), f32),
            pltpu.SemaphoreType.DMA((n,)),
            pltpu.SemaphoreType.DMA((n,)),
            pltpu.SemaphoreType.DMA((n,)),
            pltpu.SemaphoreType.DMA((n,)),
            pltpu.SemaphoreType.DMA((2 + rows // TILE,)),
            pltpu.SemaphoreType.DMA((2 + rows // TILE,)),
            pltpu.SemaphoreType.DMA((3,)),
            pltpu.SemaphoreType.DMA((n,)),
        ],
        compiler_params=pltpu.CompilerParams(
            collective_id=0, has_side_effects=True, vmem_limit_bytes=60 * 1024 * 1024
        ),
        name="sage",
    )(
        requests[0][:, None, :], table,
        near_a.T, self_a[None, :], count_a[None, :], near_b.T, self_b[None, :], count_b[None, :],
        weight_a, bias_a[None, :], weight_b, bias_b[None, :],
    )


def solution(mesh):
    placed = (
        P("dom", "mp"),
        P(None, "mp"),
        P(),
        P(None, "mp"),
        P(),
        P("dom", None, None),
        P("dom", None),
        P("dom"),
        P("dom"),
        P("dom", None),
        P("dom"),
        P("dom"),
    )
    return jax.shard_map(
        functools.partial(shards, mesh.shape["dom"]),
        mesh=mesh, in_specs=placed, out_specs=P("dom", "mp"), check_vma=False,
    )
```

```python
import functools

import jax
import jax.numpy as jnp
from jax import lax
from jax.experimental import pallas as pl
from jax.experimental.pallas import tpu as pltpu
from jax.sharding import PartitionSpec as P

MESH = pl.DeviceIdType.MESH
VMEM = pl.BlockSpec(memory_space=pltpu.VMEM)
TILE = 256


def peer(me, step, n):
    if n & (n - 1):
        return lax.rem(me + 1 + lax.rem(n // 2 - 1 + step, n - 1), n)
    return exchanged(me, n - 1 - step // 2 - lax.rem(step, 2) * (n // 2), n)


def exchanged(me, mask, n):
    other, bit = 0, 1
    while bit < n:
        other = other + lax.rem(me // bit + mask // bit, 2) * bit
        bit *= 2
    return other


def greet(me, n, partner):
    barrier = pltpu.get_barrier_semaphore()

    def one(step, carry):
        pl.semaphore_signal(
            barrier, inc=1, device_id={"dom": peer(me, step, n)}, device_id_type=MESH
        )
        return carry

    lax.fori_loop(0, n - 1, one, 0)
    if partner is not None:
        pl.semaphore_signal(barrier, inc=1, device_id={"mp": partner}, device_id_type=MESH)
    pl.semaphore_wait(barrier, n - 1 + (partner is not None))


def block_copy(source, landed, me, other, send_sem, recv_sem):
    return pltpu.make_async_remote_copy(
        src_ref=source.at[other],
        dst_ref=landed.at[me],
        send_sem=send_sem.at[other],
        recv_sem=recv_sem.at[me],
        device_id={"dom": other},
        device_id_type=MESH,
    )


def send_blocks(source, landed, me, n, send_sem, recv_sem):
    def one(step, carry):
        block_copy(source, landed, me, peer(me, step, n), send_sem, recv_sem).start()
        return carry

    lax.fori_loop(0, n - 1, one, 0)


def finish_sends(source, landed, me, n, send_sem, recv_sem):
    def one(step, carry):
        block_copy(source, landed, me, peer(me, step, n), send_sem, recv_sem).wait_send()
        return carry

    lax.fori_loop(0, n - 1, one, 0)


def wait_block(source, landed, other, recv_sem):
    pltpu.make_async_copy(source.at[other], landed.at[other], recv_sem.at[other]).wait()


def build_picks(index_ref, fan, mean_pick, own_pick):
    rows, columns = mean_pick.shape
    high = 16
    short = jnp.int16 if columns < 2**15 else jnp.int32

    def one(at, carry):
        r0 = pl.multiple_of(at * high, high)
        index = index_ref[pl.ds(r0, high), :]
        lanes = [
            jnp.broadcast_to(index[:, j : j + 1], (high, 128)).astype(short)
            for j in range(fan + 1)
        ]
        lane = lax.broadcasted_iota(jnp.int32, (high, 128), 1)
        one_value, no_value = jnp.bfloat16(1.0), jnp.bfloat16(0.0)
        for c in range(0, columns, 128):
            column = (lane + c).astype(short)
            total = jnp.where(lanes[0] == column, one_value, no_value)
            for j in range(1, fan):
                total = total + jnp.where(lanes[j] == column, one_value, no_value)
            mean_pick[pl.ds(r0, high), c : c + 128] = total
            own_pick[pl.ds(r0, high), c : c + 128] = jnp.where(
                lanes[fan] == column, one_value, no_value
            )
        return carry

    lax.fori_loop(0, rows // high, one, 0)


def dot(a, b):
    return jnp.dot(a, b, preferred_element_type=jnp.float32)


def index_rows(index, near_ref, own_ref, count_ref):
    fan, rows = near_ref.shape
    count = count_ref[...]
    pieces = [jnp.where(count > j, near_ref[j : j + 1, :], -1) for j in range(fan)]
    pieces += [own_ref[...], count, jnp.zeros((index.shape[1] - fan - 2, rows), jnp.int32)]
    index[...] = jnp.concatenate(pieces, axis=0).T


def main_kernel(
    n,
    asked_ref, table_ref, near_a_ref, self_a_ref, count_a_ref, near_b_ref, self_b_ref, count_b_ref,
    weight_a_any, bias_a_ref, weight_b_any, bias_b_ref,
    out_ref,
    table, table_wide, wanted, wanted_scalar, stage, found_ref,
    weight_a_ref, weight_b_ref, index_a_ref, index_b_ref,
    fetched, pick_a, self_pick_a, pick_b, self_pick_b, sum_mean, sum_own,
    mine_a, theirs_a, hidden, mine_b, theirs_b, mine_sq, theirs_sq,
    ask_send, ask_recv, send_sem, recv_sem, mp_send, mp_recv, load_sem, scalar_sem,
):
    me = lax.axis_index("dom")
    core = lax.axis_index("mp")
    partner = 1 - core
    each, half = found_ref.shape[1], found_ref.shape[2]
    rows = sum_mean.shape[0]
    half_hidden = hidden.shape[1]
    feature, hidden_width = weight_a_ref.shape[0] // 2, weight_b_ref.shape[0] // 2
    fan_a, fan_b = near_a_ref.shape[0], near_b_ref.shape[0]

    load_table = pltpu.make_async_copy(table_ref, table, load_sem.at[0])
    load_table.start()
    greet(me, n, partner)
    send_blocks(asked_ref, wanted, me, n, ask_send, ask_recv)
    pltpu.make_async_copy(asked_ref.at[me], wanted.at[me], ask_recv.at[me]).start()
    load_table.wait()
    load_a = pltpu.make_async_copy(weight_a_any, weight_a_ref, load_sem.at[1])
    load_a.start()
    load_b = pltpu.make_async_copy(weight_b_any, weight_b_ref, load_sem.at[2])
    load_b.start()

    def widen(tile, carry):
        at = pl.ds(pl.multiple_of(tile * 128, 128), 128)
        table_wide[at, :] = table[at, :].astype(jnp.float32)
        return carry

    lax.fori_loop(0, table.shape[0] // 128, widen, 0)
    index_rows(index_a_ref, near_a_ref, self_a_ref, count_a_ref)
    index_rows(index_b_ref, near_b_ref, self_b_ref, count_b_ref)

    def to_scalar(other):
        return pltpu.make_async_copy(wanted.at[other], wanted_scalar.at[other], scalar_sem.at[other])

    def find(other):
        to_scalar(other).wait()

        def some(at, carry):
            r0 = at * 16
            for k in range(16):
                row = wanted_scalar[other, 0, r0 + k]
                stage[pl.ds(r0 + k, 1), :] = table_wide[pl.ds(row, 1), :]
            return carry

        lax.fori_loop(0, each // 16, some, 0)
        found_ref[other] = stage[...].astype(jnp.bfloat16)

    behind = min(2, n - 1)

    def asked_of(step):
        other = peer(me, step, n)
        wait_block(asked_ref, wanted, other, ask_recv)
        to_scalar(other).start()

    def find_and_send(step, carry):
        @pl.when(step < n - 1)
        def _():
            asked_of(step)

        @pl.when(step >= behind)
        def _():
            other = peer(me, step - behind, n)
            find(other)
            block_copy(found_ref, fetched, me, other, send_sem, recv_sem).start()

        return carry

    lax.fori_loop(0, n - 1 + behind, find_and_send, 0)
    wait_block(asked_ref, wanted, me, ask_recv)
    to_scalar(me).start()
    find(me)
    pltpu.make_async_copy(found_ref.at[me], fetched.at[me], recv_sem.at[me]).start()
    build_picks(index_a_ref, fan_a, pick_a, self_pick_a)
    build_picks(index_b_ref, fan_b, pick_b, self_pick_b)
    sum_mean[...] = jnp.zeros_like(sum_mean)
    sum_own[...] = jnp.zeros_like(sum_own)
    mine_cols = pl.ds(pl.multiple_of(core * half_hidden, 128), half_hidden)
    load_a.wait()
    load_b.wait()

    per = min(n, max(1, 256 // each))
    groups = n // per
    depth = per * each

    def one_group(step, carry):
        group = exchanged(me // per, lax.rem(groups - step, groups), groups)

        def arrive(i, inner):
            wait_block(found_ref, fetched, group * per + i, recv_sem)
            return inner

        lax.fori_loop(0, per, arrive, 0)
        columns = pl.ds(pl.multiple_of(group * depth, depth), depth)

        def one_tile(tile, inner):
            at = pl.ds(pl.multiple_of(tile * TILE, TILE), TILE)
            block = fetched[pl.ds(group * per, per)].reshape(depth, half)
            sum_mean[at, :] += dot(pick_a[at, columns], block)
            sum_own[at, :] += dot(self_pick_a[at, columns], block)
            return inner

        lax.fori_loop(0, rows // TILE, one_tile, 0)
        return carry

    lax.fori_loop(0, groups, one_group, 0)

    def swap(source, landed, at):
        return pltpu.make_async_remote_copy(
            src_ref=source,
            dst_ref=landed,
            send_sem=mp_send.at[at],
            recv_sem=mp_recv.at[at],
            device_id={"mp": partner},
            device_id_type=MESH,
        )

    def rows_of(weight_ref, start, width, which):
        return weight_ref[pl.ds(pl.multiple_of(start + which * width, 128), width), :]

    def swap_a(tile):
        return swap(mine_a.at[tile], theirs_a.at[tile], 2 + tile)

    def layer_a(tile, carry):
        at = pl.ds(pl.multiple_of(tile * TILE, TILE), TILE)
        count = index_a_ref[at, fan_a + 1 : fan_a + 2].astype(jnp.float32)
        mine_a[tile, 0] = sum_own[at, :].astype(jnp.bfloat16)
        mine_a[tile, 1] = (sum_mean[at, :] / count).astype(jnp.bfloat16)
        swap_a(tile).start()
        value = dot(mine_a[tile, 0], rows_of(weight_a_ref, 0, half, core))
        value = value + dot(mine_a[tile, 1], rows_of(weight_a_ref, feature, half, core))
        sum_own[at, pl.ds(0, half_hidden)] = value
        return carry

    def layer_a_rest(tile, carry):
        at = pl.ds(pl.multiple_of(tile * TILE, TILE), TILE)
        swap_a(tile).wait()
        value = sum_own[at, pl.ds(0, half_hidden)]
        value = value + dot(theirs_a[tile, 0], rows_of(weight_a_ref, 0, half, partner))
        value = value + dot(theirs_a[tile, 1], rows_of(weight_a_ref, feature, half, partner))
        hidden[at, :] = jnp.maximum(value + bias_a_ref[:, mine_cols], 0.0).astype(jnp.bfloat16)
        return carry

    lax.fori_loop(0, rows // TILE, layer_a, 0)
    lax.fori_loop(0, rows // TILE, layer_a_rest, 0)

    mine_b[0] = dot(self_pick_b[...], hidden[...]).astype(jnp.bfloat16)
    count_b = index_b_ref[:, fan_b + 1 : fan_b + 2].astype(jnp.float32)
    mine_b[1] = (dot(pick_b[...], hidden[...]) / count_b).astype(jnp.bfloat16)
    swap_b = swap(mine_b, theirs_b, 0)
    swap_b.start()
    state = dot(mine_b[0], rows_of(weight_b_ref, 0, half_hidden, core))
    state = state + dot(mine_b[1], rows_of(weight_b_ref, hidden_width, half_hidden, core))
    swap_b.wait()
    state = state + dot(theirs_b[0], rows_of(weight_b_ref, 0, half_hidden, partner))
    state = state + dot(theirs_b[1], rows_of(weight_b_ref, hidden_width, half_hidden, partner))
    state = jnp.maximum(state + bias_b_ref[:, mine_cols], 0.0)
    mine_sq[...] = jnp.broadcast_to(jnp.sum(state * state, axis=1, keepdims=True), mine_sq.shape)
    swap_sq = swap(mine_sq, theirs_sq, 1)
    swap_sq.start()
    swap_sq.wait()
    squares = mine_sq[:, 0:1] + theirs_sq[:, 0:1]
    scale = jnp.sqrt(jnp.float32(hidden_width)) / jnp.sqrt(squares + hidden_width)
    out_ref[...] = (state * scale).astype(out_ref.dtype)
    finish_sends(asked_ref, wanted, me, n, ask_send, ask_recv)
    finish_sends(found_ref, fetched, me, n, send_sem, recv_sem)


def shards(
    n,
    table,
    weight_a,
    bias_a,
    weight_b,
    bias_b,
    requests,
    near_a,
    self_a,
    count_a,
    near_b,
    self_b,
    count_b,
):
    each = requests.shape[2]
    half, half_hidden = table.shape[1], weight_a.shape[1]
    rows, seeds, slots = near_a.shape[0], near_b.shape[0], n * each
    wide = -(-(near_a.shape[1] + 2) // 8) * 8
    bf16, f32 = jnp.bfloat16, jnp.float32
    anywhere = pl.BlockSpec(memory_space=pl.ANY)
    return pl.pallas_call(
        functools.partial(main_kernel, n),
        out_shape=jax.ShapeDtypeStruct((seeds, half_hidden), bf16),
        in_specs=[VMEM, anywhere] + [VMEM] * 6 + [anywhere, VMEM, anywhere, VMEM],
        out_specs=VMEM,
        scratch_shapes=[
            pltpu.VMEM(table.shape, bf16),
            pltpu.VMEM(table.shape, f32),
            pltpu.VMEM((n, 1, each), jnp.int32),
            pltpu.SMEM((n, 1, each), jnp.int32),
            pltpu.VMEM((each, half), f32),
            pltpu.VMEM((n, each, half), bf16),
            pltpu.VMEM(weight_a.shape, bf16),
            pltpu.VMEM(weight_b.shape, bf16),
            pltpu.VMEM((rows, wide), jnp.int32),
            pltpu.VMEM((seeds, wide), jnp.int32),
            pltpu.VMEM((n, each, half), bf16),
            pltpu.VMEM((rows, slots), bf16),
            pltpu.VMEM((rows, slots), bf16),
            pltpu.VMEM((seeds, rows), bf16),
            pltpu.VMEM((seeds, rows), bf16),
            pltpu.VMEM((rows, half), f32),
            pltpu.VMEM((rows, half), f32),
            pltpu.VMEM((rows // TILE, 2, TILE, half), bf16),
            pltpu.VMEM((rows // TILE, 2, TILE, half), bf16),
            pltpu.VMEM((rows, half_hidden), bf16),
            pltpu.VMEM((2, seeds, half_hidden), bf16),
            pltpu.VMEM((2, seeds, half_hidden), bf16),
            pltpu.VMEM((seeds, 128), f32),
            pltpu.VMEM((seeds, 128), f32),
            pltpu.SemaphoreType.DMA((n,)),
            pltpu.SemaphoreType.DMA((n,)),
            pltpu.SemaphoreType.DMA((n,)),
            pltpu.SemaphoreType.DMA((n,)),
            pltpu.SemaphoreType.DMA((2 + rows // TILE,)),
            pltpu.SemaphoreType.DMA((2 + rows // TILE,)),
            pltpu.SemaphoreType.DMA((3,)),
            pltpu.SemaphoreType.DMA((n,)),
        ],
        compiler_params=pltpu.CompilerParams(
            collective_id=0, has_side_effects=True, vmem_limit_bytes=60 * 1024 * 1024
        ),
        name="sage",
    )(
        requests[0][:, None, :], table,
        near_a.T, self_a[None, :], count_a[None, :], near_b.T, self_b[None, :], count_b[None, :],
        weight_a, bias_a[None, :], weight_b, bias_b[None, :],
    )


def solution(mesh):
    placed = (
        P("dom", "mp"),
        P(None, "mp"),
        P(),
        P(None, "mp"),
        P(),
        P("dom", None, None),
        P("dom", None),
        P("dom"),
        P("dom"),
        P("dom", None),
        P("dom"),
        P("dom"),
    )
    return jax.shard_map(
        functools.partial(shards, mesh.shape["dom"]),
        mesh=mesh, in_specs=placed, out_specs=P("dom", "mp"), check_vma=False,
    )
```
